256 devices in a mesh: pts: 32 (over x, z), grp: 8 (over y, core).
Axes of the slice: x: 4, y: 4, z: 8, core: 2. Of those that a mesh axis runs over, the one named last changes fastest.
Arguments:
- embeddings: bfloat16 [1048576, 1024], P(('pts', 'grp')), as said below
- best_start: float32 [1048576], P(('pts', 'grp')), may hold values from 0 to 2
- bounds_start: float32 [1048576], P(('pts', 'grp')), may hold values from 0 to 4
- proposals: int32 [8, 32], replicated, may hold values from 0 to 1048575
Outputs:
- gain_table: float32 [8, 32], replicated
- coverage: float32 [8], replicated
- best_final: float32 [1048576], P(('pts', 'grp'))
- bounds_final: float32 [1048576], P(('pts', 'grp'))
The draws below stay inside these ranges and needn't reach their ends.
Inputs may be any that keep to these rules, and one draw needn't show every extreme that they name: Rows are real valued embeddings of varying norm.
All inputs are finite; a program needn't handle non-finite values.
Results may differ from the reference program's by a relative error of at most 0.0003.
Values may be sent and summed in bfloat16 or wider, within the bound.
No kernel may reach another device: no remote copies, remote signals or barrier semaphores. Data moves between devices by JAX's collectives and lax.ppermute only.
A program may use at most 64 MiB of HBM per device.

```python
import jax
import jax.numpy as jnp
from jax import lax

D = 1024
PROPS = 32
STEPS = 8
POINTS = 1048576


def draw_embeddings(key, part):
    key_norm, key_scale = jax.random.split(key, 2)
    position = jnp.arange(POINTS, dtype=jnp.float32) / POINTS
    log_scale = jnp.log(3.0) * position + jax.random.uniform(key_scale, (POINTS,), jnp.float32, -0.6, 0.6)
    values = jax.random.normal(key_norm, (POINTS, D), jnp.float32)
    scaled = jnp.exp(log_scale)[:, None] * values * (0.5 * D ** (-0.25))
    return scaled.astype(jnp.bfloat16)


def plant(array, own_key, smallest, top_value):
    longest = array.shape.index(max(array.shape))
    spots = []
    for shift in (0, 1):
        where = [jax.random.randint(jax.random.fold_in(own_key, axis), (), 0, length) for axis, length in enumerate(array.shape)]
        where[longest] = (where[longest] + shift) % array.shape[longest]
        spots.append(tuple(where))
    return array.at[spots[0]].set(smallest).at[spots[1]].set(top_value)


def steps_of(key, shape, cuts, smallest, largest):
    loudness, own = 1.0, jax.random.fold_in(key, 6)
    for dim, parts in cuts:
        heights = jnp.exp(jax.random.uniform(jax.random.fold_in(own, dim), (parts,), jnp.float32, smallest / len(cuts), largest / len(cuts)))
        loudness = loudness * jnp.repeat(heights, shape[dim] // parts).reshape([-1 if axis == dim else 1 for axis in range(len(shape))])
    return loudness


def setup_inputs(seed: int = 0) -> dict:
    streams_of = jax.random.split(jax.random.key(seed), 5)
    embeddings = draw_embeddings(jax.random.fold_in(streams_of[4], 71), 0)
    best_start = jnp.clip(2.0 * jax.random.uniform(streams_of[1], (POINTS,), jnp.float32) ** steps_of(streams_of[1], (POINTS,), ((0, 256),), -0.2, 0.2), 0.0, 2.0)
    bounds_start = jnp.clip(4.0 * jax.random.uniform(streams_of[2], (POINTS,), jnp.float32) ** steps_of(streams_of[2], (POINTS,), ((0, 256),), -0.2, 0.2), 0.0, 4.0)
    proposals = plant(jax.random.randint(streams_of[3], (STEPS, PROPS), 0, POINTS), jax.random.fold_in(streams_of[3], 1), 0, POINTS - 1).astype(jnp.int32)
    return {"embeddings": embeddings, "best_start": best_start, "bounds_start": bounds_start, "proposals": proposals}


def reference(embeddings, best_start, bounds_start, proposals):
    best_sim = best_start
    bounds = bounds_start
    gain_rows = []
    cover_rows = []
    for step_index in range(STEPS):
        chosen = proposals[step_index]
        fetched = jnp.take(embeddings, chosen, axis=0)
        similarity = jnp.dot(embeddings, fetched.T, preferred_element_type=jnp.float32)
        clipped = jnp.maximum(similarity - best_sim[:, None], 0.0)
        gain_values = jnp.sum(clipped, axis=0) / POINTS
        weights = (gain_values + 0.01) / (jnp.sum(gain_values) + 0.01 * PROPS)
        mixed = jnp.dot(similarity, weights, precision=lax.Precision.HIGHEST)
        best_sim = jnp.maximum(best_sim, mixed)
        cover_rows.append(jnp.sum(best_sim) / POINTS)
        bounds = bounds.at[chosen].set(gain_values)
        gain_rows.append(gain_values)
    return jnp.stack(gain_rows), jnp.stack(cover_rows), best_sim, bounds
```

```python
import functools

import jax
import jax.numpy as jnp
from jax import lax
from jax.experimental import pallas as pl
from jax.experimental.pallas import tpu as pltpu
from jax.sharding import Mesh
from jax.sharding import PartitionSpec as P

AXES = ("x", "z", "y", "core")
VMEM = pl.BlockSpec(memory_space=pltpu.VMEM)
SMEM = pl.BlockSpec(memory_space=pltpu.SMEM)
ANY = pl.BlockSpec(memory_space=pl.ANY)
LANES = 128
SUB = 8
GRANT = 12 << 20
STREAM_GRANT = 48 << 20
CHUNK = 512


def shape_of(shape, dtype=jnp.float32):
    return jax.ShapeDtypeStruct(shape, dtype)


def rows_kernel(offsets, points, out, blocks, rows, arrived):
    count, row_total = out.shape[0], points.shape[0]

    def owned(k):
        return (offsets[k] >= 0) & (offsets[k] < row_total)

    def copy(k):
        base = pl.multiple_of(lax.shift_right_logical(offsets[k], 3) * SUB, SUB)
        return pltpu.make_async_copy(points.at[pl.ds(base, SUB)], blocks.at[k], arrived.at[k])

    def start(k, carry):
        @pl.when(owned(k))
        def _():
            copy(k).start()

        return carry

    def take(k, carry):
        @pl.when(owned(k))
        def _():
            copy(k).wait()
            block = blocks[k].astype(jnp.float32)
            line = lax.broadcasted_iota(jnp.int32, block.shape, 0)
            mine = jnp.where(line == (offsets[k] & (SUB - 1)), block, 0.0)
            rows[pl.ds(k, 1), :] = jnp.sum(mine, axis=0, keepdims=True)

        return carry

    lax.fori_loop(0, count, start, 0, unroll=8)
    rows[...] = jnp.zeros_like(rows)
    lax.fori_loop(0, count, take, 0, unroll=8)
    out[...] = rows[...].astype(out.dtype)


def own_rows(offsets, points):
    count, width = offsets.shape[0], points.shape[1]
    return pl.pallas_call(
        rows_kernel,
        out_shape=shape_of((count, width), points.dtype),
        in_specs=[SMEM, ANY],
        out_specs=VMEM,
        scratch_shapes=[
            pltpu.VMEM((count, SUB, width), points.dtype),
            pltpu.VMEM((count, width), jnp.float32),
            pltpu.SemaphoreType.DMA((count,)),
        ],
        compiler_params=pltpu.CompilerParams(vmem_limit_bytes=STREAM_GRANT),
    )(offsets, points)


def as_column(row, height):
    line = lax.broadcasted_iota(jnp.int32, (height, LANES), 0)
    lane = lax.broadcasted_iota(jnp.int32, (height, LANES), 1)
    spread = jnp.where(line == lane, jnp.broadcast_to(row, (height, LANES)), 0.0)
    return jnp.sum(spread, axis=1, keepdims=True)


def as_row(column):
    height = column.shape[0]
    line = lax.broadcasted_iota(jnp.int32, (height, LANES), 0)
    lane = lax.broadcasted_iota(jnp.int32, (height, LANES), 1)
    return jnp.sum(jnp.where(line == lane, column, 0.0), axis=0, keepdims=True)


def every_sublane(tile):
    for shift in (4, 2, 1):
        tile = tile + pltpu.roll(tile, shift, 0)
    return tile


def shares(gained, cover, props):
    lane = lax.broadcasted_iota(jnp.int32, (1, LANES), 1)
    row = as_row(jnp.sum(gained, axis=1, keepdims=True))
    total = jnp.sum(cover[:1], axis=1, keepdims=True)
    return jnp.where(lane == props, total, row)


def first_kernel(props, fetched, points, best, similarity, out, held, arrived):
    width = best.shape[1]
    chunks = []
    for i in range(0, width, CHUNK):
        part = pl.ds(i, CHUNK)
        chunks.append(pltpu.make_async_copy(points.at[part], held.at[part], arrived.at[i // CHUNK]))
        chunks[-1].start()
    gained = jnp.zeros((props, LANES), jnp.float32)
    for i, chunk in zip(range(0, width, CHUNK), chunks):
        chunk.wait()
        similarity[:, i : i + CHUNK] = lax.dot_general(
            fetched[...],
            held[i : i + CHUNK, :],
            (((1,), (1,)), ((), ())),
            preferred_element_type=jnp.float32,
        )
        for j in range(i, i + CHUNK, LANES):
            cols = slice(j, j + LANES)
            gained += jnp.maximum(similarity[0:props, cols] - best[:, cols], 0.0)
    row = shares(gained, jnp.zeros((SUB, LANES), jnp.float32), props)
    out[...] = jnp.broadcast_to(row, out.shape)


def first_call(props, fetched, points, best, devices):
    return pl.pallas_call(
        functools.partial(first_kernel, props),
        out_shape=[shape_of((fetched.shape[0], best.shape[1])), shape_of((devices, LANES))],
        in_specs=[VMEM, ANY, VMEM],
        out_specs=[VMEM, VMEM],
        scratch_shapes=[
            pltpu.VMEM(points.shape, points.dtype),
            pltpu.SemaphoreType.DMA((points.shape[0] // CHUNK,)),
        ],
        compiler_params=pltpu.CompilerParams(vmem_limit_bytes=STREAM_GRANT),
    )(fetched, points, best)


def step_kernel(step, props, point_total, parts, similarity, best, table, new_best, new_table, out=None):
    width = best.shape[1]
    last = out is None
    lane = lax.broadcasted_iota(jnp.int32, (1, LANES), 1)
    line = lax.broadcasted_iota(jnp.int32, table.shape, 0)
    gains = jnp.sum(parts[...], axis=0, keepdims=True) / point_total
    new_table[...] = jnp.where(line == step, gains, table[...])
    total = jnp.sum(jnp.where(lane < props, gains, 0.0), axis=1, keepdims=True)
    weight = as_column((gains + 0.01) / (total + 0.01 * props), props)
    weights = jnp.broadcast_to(weight, (props, LANES))
    here = slice(step * props, (step + 1) * props)
    following = slice((step + 1) * props, (step + 2) * props)
    gained = jnp.zeros((props, LANES), jnp.float32)
    cover = jnp.zeros((SUB, LANES), jnp.float32)
    for j in range(width // LANES):
        cols = slice(j * LANES, (j + 1) * LANES)
        product = similarity[here, cols] * weights
        mixed = product[0:SUB]
        for i in range(SUB, props, SUB):
            mixed = mixed + product[i : i + SUB]
        now = jnp.maximum(jnp.broadcast_to(best[:, cols], (SUB, LANES)), every_sublane(mixed))
        new_best[:, cols] = now[: new_best.shape[0]]
        cover += now
        if not last:
            ahead = jnp.concatenate([now] * (props // SUB), axis=0)
            gained += jnp.maximum(similarity[following, cols] - ahead, 0.0)
    return shares(gained, cover, props)


def middle_kernel(step, props, point_total, parts, similarity, best, table, new_best, new_table, out):
    row = step_kernel(step, props, point_total, parts, similarity, best, table, new_best, new_table, out)
    out[...] = jnp.broadcast_to(row, out.shape)


def last_kernel(step, props, point_total, parts, similarity, best, table, new_best, new_table, out):
    row = step_kernel(step, props, point_total, parts, similarity, best, table, new_best, new_table)
    out[...] = jnp.broadcast_to(row, out.shape)


def cover_kernel(props, point_total, parts, table, gain_table, coverage):
    steps = table.shape[0]
    gain_table[...] = table[:, 0:props]
    final = jnp.sum(parts[...], axis=0, keepdims=True) / point_total
    line = lax.broadcasted_iota(jnp.int32, table.shape, 0)
    lane = lax.broadcasted_iota(jnp.int32, table.shape, 1)
    ahead = jnp.where(line == steps - 1, final, pltpu.roll(table[...], steps - 1, 0))
    column = jnp.sum(jnp.where(lane == props, ahead, 0.0), axis=1, keepdims=True)
    coverage[...] = as_row(column)[:, 0:steps]


def bounds_kernel(offsets, table, bounds, out):
    steps, props = table.shape[0], offsets.shape[0] // table.shape[0]
    out[...] = bounds[...]
    row_total = out.shape[0] * LANES

    def put(k, carry):
        offset = offsets[k]

        @pl.when((offset >= 0) & (offset < row_total))
        def _():
            step, prop = lax.div(k, props), lax.rem(k, props)
            lane = lax.broadcasted_iota(jnp.int32, (1, LANES), 1)
            gains = table[pl.ds(step, 1), :]
            gain = jnp.sum(jnp.where(lane == prop, gains, 0.0), axis=1, keepdims=True)
            at = pl.ds(lax.shift_right_logical(offset, 7), 1)
            out[at, :] = jnp.where(lane == (offset & (LANES - 1)), gain, out[at, :])

        return carry

    lax.fori_loop(0, offsets.shape[0], put, 0, unroll=8)


def call(kernel, out_shape, in_specs):
    many = isinstance(out_shape, (tuple, list))
    return pl.pallas_call(
        kernel,
        out_shape=out_shape,
        in_specs=in_specs,
        out_specs=[VMEM] * len(out_shape) if many else VMEM,
        compiler_params=pltpu.CompilerParams(vmem_limit_bytes=GRANT),
    )


def every_part(parts):
    return lax.all_to_all(parts.reshape(parts.shape[0], 1, LANES), AXES, 0, 0, tiled=True).reshape(parts.shape)


def arrived_sum(rows, axes):
    tiles = lax.all_to_all(
        rows.reshape(lax.axis_size(axes), -1, rows.shape[1]), axes, 0, 0, tiled=True
    )
    return jnp.sum(tiles.astype(jnp.float32), axis=0).astype(rows.dtype)


def copies(rows, axes):
    sent = jnp.broadcast_to(rows, (lax.axis_size(axes), *rows.shape))
    return lax.all_to_all(sent, axes, 0, 0, tiled=True).reshape(-1, rows.shape[1])


def on_device(embeddings, best_start, bounds_start, proposals):
    row_count, devices = embeddings.shape[0], lax.axis_size(AXES)
    steps, props = proposals.shape
    point_total = row_count * devices
    offsets = proposals.reshape(-1) - lax.axis_index(AXES) * row_count

    rows = own_rows(offsets, embeddings)
    rows = arrived_sum(rows, ("x", "y", "core"))
    rows = arrived_sum(jnp.tile(rows, (lax.axis_size("z"), 1)), "z")
    fetched = copies(rows, ("x", "y", "core"))
    best = best_start.reshape(1, row_count)
    table = jnp.zeros((steps, LANES), jnp.float32)
    line = shape_of((devices, LANES))
    similarity, parts = first_call(props, fetched, embeddings, best, devices)
    for step in range(steps):
        parts = every_part(parts)
        last = step == steps - 1
        best, table, parts = call(
            functools.partial(last_kernel if last else middle_kernel, step, props, point_total),
            [shape_of((1 if last else SUB, row_count)), shape_of(table.shape), line],
            [VMEM] * 4,
        )(parts, similarity, best, table)
    bounds = call(bounds_kernel, shape_of((row_count // LANES, LANES)), [SMEM, VMEM, VMEM])(
        offsets, table, bounds_start.reshape(-1, LANES)
    )
    gain_table, coverage = call(
        functools.partial(cover_kernel, props, point_total),
        [shape_of((steps, props)), shape_of((1, steps))],
        [VMEM] * 2,
    )(every_part(parts), table)
    return gain_table, coverage.reshape(-1), best.reshape(-1), bounds.reshape(-1)


def solution(mesh):
    torus = Mesh(mesh.devices.reshape(4, 8, 4, 2), AXES)
    in_specs = (P(AXES, None), P(AXES), P(AXES), P())
    out_specs = (P(), P(), P(AXES), P(AXES))
    return jax.shard_map(
        on_device, mesh=torus, in_specs=in_specs, out_specs=out_specs, check_vma=False
    )
```

```python
import functools

import jax
import jax.numpy as jnp
from jax import lax
from jax.experimental import pallas as pl
from jax.experimental.pallas import tpu as pltpu
from jax.sharding import Mesh
from jax.sharding import PartitionSpec as P

AXIS = "device"
X, Z, Y, CORES = 4, 8, 4, 2
VMEM = pl.BlockSpec(memory_space=pltpu.VMEM)
SMEM = pl.BlockSpec(memory_space=pltpu.SMEM)
ANY = pl.BlockSpec(memory_space=pl.ANY)
LANES = 128
SUB = 8
GRANT = 12 << 20
ROWS_GRANT = 46 << 20
CHUNK = 512
WAITS = pl.CostEstimate(flops=200_000_000_000, bytes_accessed=1_000_000_000, transcendentals=0)


def shape_of(shape, dtype=jnp.float32):
    return jax.ShapeDtypeStruct(shape, dtype)


def first_row(row_total):
    return lax.axis_index(AXIS) * row_total


def rows_kernel(proposals, points, mine, others, owned, blocks, rows, arrived):
    row_total = points.shape[0]
    steps, props = proposals.shape
    half = mine.shape[0]
    lists, room = owned.shape
    first = first_row(row_total)

    def offset_of(k):
        return proposals[lax.div(k, props), lax.rem(k, props)] - first

    def note(i, found):
        found = list(found)
        for prop in range(props):
            for part in range(lists):
                step = part * (steps // lists) + i
                offset = proposals[step, prop] - first
                owned[part, found[part]] = step * props + prop
                found[part] += jnp.where((offset >= 0) & (offset < row_total), 1, 0)
        return tuple(found)

    def copy(k):
        base = pl.multiple_of(lax.shift_right_logical(offset_of(k), 3) * SUB, SUB)
        return pltpu.make_async_copy(points.at[pl.ds(base, SUB)], blocks.at[k], arrived.at[k])

    found = lax.fori_loop(0, steps // lists, note, (jnp.int32(0),) * lists)
    for part in range(lists):

        def start(i, carry, part=part):
            copy(owned[part, i]).start()
            return carry

        lax.fori_loop(0, found[part], start, 0)
    rows[...] = jnp.zeros_like(rows)
    for part in range(lists):

        def take(i, carry, part=part):
            k = owned[part, i]
            copy(k).wait()
            block = blocks[k].astype(jnp.float32)
            line = lax.broadcasted_iota(jnp.int32, block.shape, 0)
            row = jnp.where(line == (offset_of(k) & (SUB - 1)), block, 0.0)
            rows[pl.ds(k, 1), :] = jnp.sum(row, axis=0, keepdims=True)
            return carry

        lax.fori_loop(0, found[part], take, 0)
    core = lax.rem(lax.axis_index(AXIS), CORES)
    at = pl.multiple_of(core * half, half)
    mine[...] = rows[pl.ds(at, half), :].astype(mine.dtype)
    at = pl.multiple_of((1 - core) * half, half)
    others[...] = rows[pl.ds(at, half), :].astype(others.dtype)


def own_rows(proposals, points):
    count, width = proposals.size, points.shape[1]
    half = shape_of((count // CORES, width), points.dtype)
    return pl.pallas_call(
        rows_kernel,
        out_shape=[half, half],
        in_specs=[SMEM, ANY],
        out_specs=[VMEM, VMEM],
        scratch_shapes=[
            pltpu.SMEM((4, count // 4 + 1), jnp.int32),
            pltpu.VMEM((count, SUB, width), points.dtype),
            pltpu.VMEM((count, width), jnp.float32),
            pltpu.SemaphoreType.DMA((count,)),
        ],
        compiler_params=pltpu.CompilerParams(vmem_limit_bytes=ROWS_GRANT),
    )(proposals, points)


def pair_kernel(mine, arrived, out):
    out[...] = mine[...] + arrived[...]


def sum_kernel(tiles, out):
    total = tiles[0].astype(jnp.float32)
    for i in range(1, tiles.shape[0]):
        total += tiles[i].astype(jnp.float32)
    total = total.astype(out.dtype)
    for i in range(out.shape[0]):
        out[i] = total


def summed(tiles, copies):
    return call(sum_kernel, shape_of((copies, *tiles.shape[1:]), tiles.dtype), [VMEM], WAITS)(tiles)


def device(x, z, y, core):
    return ((x * Z + z) * Y + y) * CORES + core


PLANES = [[device(x, z, y, c) for x in range(X) for y in range(Y)] for z in range(Z) for c in range(CORES)]
LINES = [[device(x, z, y, c) for z in range(Z)] for x in range(X) for y in range(Y) for c in range(CORES)]
CHIPS = [(i, i ^ 1) for i in range(X * Z * Y * CORES)]


def back_and_forth(sizes):
    if not sizes:
        return [()]
    inner = back_and_forth(sizes[1:])
    return [(i, *rest) for i in range(sizes[0]) for rest in (inner if i % 2 == 0 else inner[::-1])]


ALL = [[device(x, z, y, c) for z, x, y, c in back_and_forth((Z, X, Y, CORES))]]


def exchanged(tiles, groups):
    return lax.all_to_all(tiles, AXIS, 0, 0, tiled=True, axis_index_groups=groups)


def from_other_core(rows):
    return lax.ppermute(rows, AXIS, CHIPS)


def as_column(row, height):
    line = lax.broadcasted_iota(jnp.int32, (height, LANES), 0)
    lane = lax.broadcasted_iota(jnp.int32, (height, LANES), 1)
    spread = jnp.where(line == lane, jnp.broadcast_to(row, (height, LANES)), 0.0)
    return jnp.sum(spread, axis=1, keepdims=True)


def as_row(column):
    height = column.shape[0]
    line = lax.broadcasted_iota(jnp.int32, (height, LANES), 0)
    lane = lax.broadcasted_iota(jnp.int32, (height, LANES), 1)
    return jnp.sum(jnp.where(line == lane, column, 0.0), axis=0, keepdims=True)


def every_sublane(tile):
    for shift in (4, 2, 1):
        tile = tile + pltpu.roll(tile, shift, 0)
    return tile


def shares(gained, cover, props):
    lane = lax.broadcasted_iota(jnp.int32, (1, LANES), 1)
    row = as_row(jnp.sum(gained, axis=1, keepdims=True))
    total = jnp.sum(cover[:1], axis=1, keepdims=True)
    return jnp.where(lane == props, total, row)


def first_kernel(props, mine, others, points, best, similarity, out, fetched):
    width, half = best.shape[1], mine.shape[0]
    core = lax.rem(lax.axis_index(AXIS), CORES)
    fetched[pl.ds(pl.multiple_of(core * half, half), half), :] = mine[...]
    fetched[pl.ds(pl.multiple_of((1 - core) * half, half), half), :] = others[...]
    gained = jnp.zeros((props, LANES), jnp.float32)
    for i in range(0, width, CHUNK):
        similarity[:, i : i + CHUNK] = lax.dot_general(
            fetched[...],
            points[i : i + CHUNK, :],
            (((1,), (1,)), ((), ())),
            preferred_element_type=jnp.float32,
        )
        for j in range(i, i + CHUNK, LANES):
            cols = slice(j, j + LANES)
            gained += jnp.maximum(similarity[0:props, cols] - best[:, cols], 0.0)
    row = shares(gained, jnp.zeros((SUB, LANES), jnp.float32), props)
    out[...] = jnp.broadcast_to(row, out.shape)


def step_kernel(step, props, point_total, parts, similarity, best, table, new_best, new_table, out=None):
    width = best.shape[1]
    last = out is None
    lane = lax.broadcasted_iota(jnp.int32, (1, LANES), 1)
    line = lax.broadcasted_iota(jnp.int32, table.shape, 0)
    gains = jnp.sum(parts[...], axis=0, keepdims=True) / point_total
    new_table[...] = jnp.where(line == step, gains, table[...])
    total = jnp.sum(jnp.where(lane < props, gains, 0.0), axis=1, keepdims=True)
    weight = as_column((gains + 0.01) / (total + 0.01 * props), props)
    weights = jnp.broadcast_to(weight, (props, LANES))
    here = slice(step * props, (step + 1) * props)
    following = slice((step + 1) * props, (step + 2) * props)
    gained = jnp.zeros((props, LANES), jnp.float32)
    cover = jnp.zeros((SUB, LANES), jnp.float32)
    for j in range(width // LANES):
        cols = slice(j * LANES, (j + 1) * LANES)
        product = similarity[here, cols] * weights
        mixed = product[0:SUB]
        for i in range(SUB, props, SUB):
            mixed = mixed + product[i : i + SUB]
        now = jnp.maximum(jnp.broadcast_to(best[:, cols], (SUB, LANES)), every_sublane(mixed))
        new_best[:, cols] = now[: new_best.shape[0]]
        cover += now
        if not last:
            ahead = jnp.concatenate([now] * (props // SUB), axis=0)
            gained += jnp.maximum(similarity[following, cols] - ahead, 0.0)
    return shares(gained, cover, props)


def middle_kernel(step, props, point_total, parts, similarity, best, table, new_best, new_table, out):
    row = step_kernel(step, props, point_total, parts, similarity, best, table, new_best, new_table, out)
    out[...] = jnp.broadcast_to(row, out.shape)


def last_kernel(step, props, point_total, parts, similarity, best, table, new_best, new_table, out):
    row = step_kernel(step, props, point_total, parts, similarity, best, table, new_best, new_table)
    out[...] = jnp.broadcast_to(row, out.shape)


def cover_kernel(props, point_total, parts, table, gain_table, coverage):
    steps = table.shape[0]
    gain_table[...] = table[:, 0:props]
    final = jnp.sum(parts[...], axis=0, keepdims=True) / point_total
    line = lax.broadcasted_iota(jnp.int32, table.shape, 0)
    lane = lax.broadcasted_iota(jnp.int32, table.shape, 1)
    ahead = jnp.where(line == steps - 1, final, pltpu.roll(table[...], steps - 1, 0))
    column = jnp.sum(jnp.where(lane == props, ahead, 0.0), axis=1, keepdims=True)
    coverage[...] = as_row(column)[:, 0:steps]


def bounds_kernel(proposals, table, bounds, out):
    steps, props = proposals.shape
    out[...] = bounds[...]
    row_total = out.shape[0] * LANES
    first = first_row(row_total)
    lane = lax.broadcasted_iota(jnp.int32, (1, LANES), 1)

    def put(step, carry):
        for prop in range(props):
            offset = proposals[step, prop] - first

            @pl.when((offset >= 0) & (offset < row_total))
            def _():
                gains = table[pl.ds(step, 1), :]
                gain = jnp.sum(jnp.where(lane == prop, gains, 0.0), axis=1, keepdims=True)
                at = pl.ds(lax.shift_right_logical(offset, 7), 1)
                out[at, :] = jnp.where(lane == (offset & (LANES - 1)), gain, out[at, :])

        return carry

    lax.fori_loop(0, steps, put, 0)


def call(kernel, out_shape, in_specs, cost=None, scratch=()):
    many = isinstance(out_shape, (tuple, list))
    return pl.pallas_call(
        kernel,
        out_shape=out_shape,
        in_specs=in_specs,
        out_specs=[VMEM] * len(out_shape) if many else VMEM,
        compiler_params=pltpu.CompilerParams(vmem_limit_bytes=GRANT),
        cost_estimate=cost,
        scratch_shapes=scratch,
    )


def every_part(parts):
    return exchanged(parts.reshape(parts.shape[0], 1, LANES), ALL).reshape(parts.shape)


def on_device(embeddings, best_start, bounds_start, proposals):
    row_count, devices = embeddings.shape[0], lax.axis_size(AXIS)
    steps, props = proposals.shape
    point_total = row_count * devices

    mine, others = own_rows(proposals, embeddings)
    half = shape_of(mine.shape, mine.dtype)
    tiles = call(pair_kernel, half, [VMEM] * 2)(mine, from_other_core(others))
    tiles = exchanged(tiles.reshape(X * Y, -1, mine.shape[1]), PLANES)
    tiles = exchanged(summed(tiles, Z), LINES)
    mine = exchanged(summed(tiles, X * Y), PLANES).reshape(mine.shape)
    others = from_other_core(mine)

    best = best_start.reshape(1, row_count)
    table = jnp.zeros((steps, LANES), jnp.float32)
    line = shape_of((devices, LANES))
    similarity, parts = call(
        functools.partial(first_kernel, props),
        [shape_of((steps * props, row_count)), line],
        [VMEM] * 4,
        scratch=[pltpu.VMEM((steps * props, mine.shape[1]), mine.dtype)],
    )(mine, others, embeddings, best)
    for step in range(steps):
        parts = every_part(parts)
        last = step == steps - 1
        best, table, parts = call(
            functools.partial(last_kernel if last else middle_kernel, step, props, point_total),
            [shape_of((1 if last else SUB, row_count)), shape_of(table.shape), line],
            [VMEM] * 4,
        )(parts, similarity, best, table)
    bounds = call(bounds_kernel, shape_of((row_count // LANES, LANES)), [SMEM, VMEM, VMEM])(
        proposals, table, bounds_start.reshape(-1, LANES)
    )
    gain_table, coverage = call(
        functools.partial(cover_kernel, props, point_total),
        [shape_of((steps, props)), shape_of((1, steps))],
        [VMEM] * 2,
    )(every_part(parts), table)
    return gain_table, coverage.reshape(-1), best.reshape(-1), bounds.reshape(-1)


def solution(mesh):
    line = Mesh(mesh.devices.reshape(-1), (AXIS,))
    in_specs = (P(AXIS, None), P(AXIS), P(AXIS), P())
    out_specs = (P(), P(), P(AXIS), P(AXIS))
    return jax.shard_map(
        on_device, mesh=line, in_specs=in_specs, out_specs=out_specs, check_vma=False
    )
```

```python
import functools

import jax
import jax.numpy as jnp
from jax import lax
from jax.experimental import pallas as pl
from jax.experimental.pallas import tpu as pltpu
from jax.sharding import Mesh
from jax.sharding import PartitionSpec as P

AXIS = "device"
X, Z, Y, CORES = 4, 8, 4, 2
VMEM = pl.BlockSpec(memory_space=pltpu.VMEM)
SMEM = pl.BlockSpec(memory_space=pltpu.SMEM)
ANY = pl.BlockSpec(memory_space=pl.ANY)
LANES = 128
SUB = 8
GRANT = 12 << 20
ROWS_GRANT = 46 << 20
CHUNK = 512
LISTS, SLOTS = 4, 4
WAITS = pl.CostEstimate(flops=200_000_000_000, bytes_accessed=1_000_000_000, transcendentals=0)


def shape_of(shape, dtype=jnp.float32):
    return jax.ShapeDtypeStruct(shape, dtype)


def first_row(row_total):
    return lax.axis_index(AXIS) * row_total


def rows_kernel(proposals, points, mine, others, owned, blocks, rows, arrived):
    row_total = points.shape[0]
    steps, props = proposals.shape
    half = mine.shape[0]
    lists, slots = arrived.shape
    first = first_row(row_total)

    def offset_of(k):
        return proposals[lax.div(k, props), lax.rem(k, props)] - first

    def note(i, found):
        found = list(found)
        for prop in range(props):
            for part in range(lists):
                step = part * (steps // lists) + i
                offset = proposals[step, prop] - first
                owned[part, found[part]] = step * props + prop
                found[part] += jnp.where((offset >= 0) & (offset < row_total), 1, 0)
        return tuple(found)

    def copy(k, part, slot):
        base = pl.multiple_of(lax.shift_right_logical(offset_of(k), 3) * SUB, SUB)
        return pltpu.make_async_copy(
            points.at[pl.ds(base, SUB)], blocks.at[part, slot], arrived.at[part, slot]
        )

    found = lax.fori_loop(0, steps // lists, note, (jnp.int32(0),) * lists)
    rows[...] = jnp.zeros_like(rows)

    def batch(b, carry):
        done = b * slots
        counts = [jnp.clip(found[part] - done, 0, slots) for part in range(lists)]
        for part in range(lists):

            def start(slot, carry, part=part):
                copy(owned[part, done + slot], part, slot).start()
                return carry

            lax.fori_loop(0, counts[part], start, 0)
        for part in range(lists):

            def take(slot, carry, part=part):
                k = owned[part, done + slot]
                copy(k, part, slot).wait()
                block = blocks[part, slot].astype(jnp.float32)
                line = lax.broadcasted_iota(jnp.int32, block.shape, 0)
                row = jnp.where(line == (offset_of(k) & (SUB - 1)), block, 0.0)
                rows[pl.ds(k, 1), :] = jnp.sum(row, axis=0, keepdims=True)
                return carry

            lax.fori_loop(0, counts[part], take, 0)
        return carry

    longest = functools.reduce(jnp.maximum, found)
    lax.fori_loop(0, lax.div(longest + slots - 1, slots), batch, 0)
    core = lax.rem(lax.axis_index(AXIS), CORES)
    at = pl.multiple_of(core * half, half)
    mine[...] = rows[pl.ds(at, half), :].astype(mine.dtype)
    at = pl.multiple_of((1 - core) * half, half)
    others[...] = rows[pl.ds(at, half), :].astype(others.dtype)


def own_rows(proposals, points):
    count, width = proposals.size, points.shape[1]
    half = shape_of((count // CORES, width), points.dtype)
    return pl.pallas_call(
        rows_kernel,
        out_shape=[half, half],
        in_specs=[SMEM, ANY],
        out_specs=[VMEM, VMEM],
        scratch_shapes=[
            pltpu.SMEM((LISTS, count // LISTS + 1), jnp.int32),
            pltpu.VMEM((LISTS, SLOTS, SUB, width), points.dtype),
            pltpu.VMEM((count, width), jnp.float32),
            pltpu.SemaphoreType.DMA((LISTS, SLOTS)),
        ],
        compiler_params=pltpu.CompilerParams(vmem_limit_bytes=ROWS_GRANT),
    )(proposals, points)


def pair_kernel(mine, arrived, out):
    out[...] = mine[...] + arrived[...]


def sum_kernel(tiles, out):
    total = tiles[0].astype(jnp.float32)
    for i in range(1, tiles.shape[0]):
        total += tiles[i].astype(jnp.float32)
    total = total.astype(out.dtype)
    for i in range(out.shape[0]):
        out[i] = total


def summed(tiles, copies):
    return call(sum_kernel, shape_of((copies, *tiles.shape[1:]), tiles.dtype), [VMEM], WAITS)(tiles)


def device(x, z, y, core):
    return ((x * Z + z) * Y + y) * CORES + core


PLANES = [[device(x, z, y, c) for x in range(X) for y in range(Y)] for z in range(Z) for c in range(CORES)]
LINES = [[device(x, z, y, c) for z in range(Z)] for x in range(X) for y in range(Y) for c in range(CORES)]
CHIPS = [(i, i ^ 1) for i in range(X * Z * Y * CORES)]


def back_and_forth(sizes):
    if not sizes:
        return [()]
    inner = back_and_forth(sizes[1:])
    return [(i, *rest) for i in range(sizes[0]) for rest in (inner if i % 2 == 0 else inner[::-1])]


ALL = [[device(x, z, y, c) for z, x, y, c in back_and_forth((Z, X, Y, CORES))]]


def exchanged(tiles, groups):
    return lax.all_to_all(tiles, AXIS, 0, 0, tiled=True, axis_index_groups=groups)


def from_other_core(rows):
    return lax.ppermute(rows, AXIS, CHIPS)


def as_column(row, height):
    line = lax.broadcasted_iota(jnp.int32, (height, LANES), 0)
    lane = lax.broadcasted_iota(jnp.int32, (height, LANES), 1)
    spread = jnp.where(line == lane, jnp.broadcast_to(row, (height, LANES)), 0.0)
    return jnp.sum(spread, axis=1, keepdims=True)


def as_row(column):
    height = column.shape[0]
    line = lax.broadcasted_iota(jnp.int32, (height, LANES), 0)
    lane = lax.broadcasted_iota(jnp.int32, (height, LANES), 1)
    return jnp.sum(jnp.where(line == lane, column, 0.0), axis=0, keepdims=True)


def every_sublane(tile):
    for shift in (4, 2, 1):
        tile = tile + pltpu.roll(tile, shift, 0)
    return tile


def shares(gained, cover):
    return as_row(jnp.sum(jnp.concatenate([gained, cover], axis=0), axis=1, keepdims=True))


def first_kernel(props, mine, others, points, best, similarity, out, fetched):
    width, half = best.shape[1], mine.shape[0]
    core = lax.rem(lax.axis_index(AXIS), CORES)
    fetched[pl.ds(pl.multiple_of(core * half, half), half), :] = mine[...]
    fetched[pl.ds(pl.multiple_of((1 - core) * half, half), half), :] = others[...]
    gained = jnp.zeros((props, LANES), jnp.float32)
    for i in range(0, width, CHUNK):
        similarity[:, i : i + CHUNK] = lax.dot_general(
            fetched[...],
            points[i : i + CHUNK, :],
            (((1,), (1,)), ((), ())),
            preferred_element_type=jnp.float32,
        )
        for j in range(i, i + CHUNK, LANES):
            cols = slice(j, j + LANES)
            gained += jnp.maximum(similarity[0:props, cols] - best[:, cols], 0.0)
    row = shares(gained, jnp.zeros((SUB, LANES), jnp.float32))
    out[...] = jnp.broadcast_to(row, out.shape)


def step_kernel(step, props, point_total, parts, similarity, best, table, new_best, new_table, out=None):
    width = best.shape[1]
    last = out is None
    lane = lax.broadcasted_iota(jnp.int32, (1, LANES), 1)
    line = lax.broadcasted_iota(jnp.int32, table.shape, 0)
    gains = jnp.sum(parts[...], axis=0, keepdims=True) / point_total
    new_table[...] = jnp.where(line == step, gains, table[...])
    total = jnp.sum(jnp.where(lane < props, gains, 0.0), axis=1, keepdims=True)
    whole = jnp.broadcast_to(1.0 / (total + 0.01 * props), (SUB, LANES))
    share = jnp.broadcast_to(as_column(gains + 0.01, props), (props, LANES))
    here = slice(step * props, (step + 1) * props)
    following = slice((step + 1) * props, (step + 2) * props)
    gained = jnp.zeros((props, LANES), jnp.float32)
    cover = jnp.zeros((SUB, LANES), jnp.float32)
    for j in range(width // LANES):
        cols = slice(j * LANES, (j + 1) * LANES)
        product = similarity[here, cols] * share
        mixed = product[0:SUB]
        for i in range(SUB, props, SUB):
            mixed = mixed + product[i : i + SUB]
        now = jnp.maximum(jnp.broadcast_to(best[:, cols], (SUB, LANES)), every_sublane(mixed) * whole)
        new_best[:, cols] = now[: new_best.shape[0]]
        cover += now
        if not last:
            ahead = jnp.concatenate([now] * (props // SUB), axis=0)
            gained += jnp.maximum(similarity[following, cols] - ahead, 0.0)
    return shares(gained, cover)


def middle_kernel(step, props, point_total, parts, similarity, best, table, new_best, new_table, out):
    row = step_kernel(step, props, point_total, parts, similarity, best, table, new_best, new_table, out)
    out[...] = jnp.broadcast_to(row, out.shape)


def last_kernel(step, props, point_total, parts, similarity, best, table, new_best, new_table, out):
    row = step_kernel(step, props, point_total, parts, similarity, best, table, new_best, new_table)
    out[...] = jnp.broadcast_to(row, out.shape)


def cover_kernel(props, point_total, parts, table, gain_table, coverage):
    steps = table.shape[0]
    gain_table[...] = table[:, 0:props]
    final = jnp.sum(parts[...], axis=0, keepdims=True) / point_total
    line = lax.broadcasted_iota(jnp.int32, table.shape, 0)
    lane = lax.broadcasted_iota(jnp.int32, table.shape, 1)
    ahead = jnp.where(line == steps - 1, final, pltpu.roll(table[...], steps - 1, 0))
    column = jnp.sum(jnp.where(lane == props, ahead, 0.0), axis=1, keepdims=True)
    coverage[...] = as_row(column)[:, 0:steps]


def bounds_kernel(proposals, table, bounds, out):
    steps, props = proposals.shape
    out[...] = bounds[...]
    row_total = out.shape[0] * LANES
    first = first_row(row_total)
    lane = lax.broadcasted_iota(jnp.int32, (1, LANES), 1)

    def put(step, carry):
        for prop in range(props):
            offset = proposals[step, prop] - first

            @pl.when((offset >= 0) & (offset < row_total))
            def _():
                gains = table[pl.ds(step, 1), :]
                gain = jnp.sum(jnp.where(lane == prop, gains, 0.0), axis=1, keepdims=True)
                at = pl.ds(lax.shift_right_logical(offset, 7), 1)
                out[at, :] = jnp.where(lane == (offset & (LANES - 1)), gain, out[at, :])

        return carry

    lax.fori_loop(0, steps, put, 0)


def call(kernel, out_shape, in_specs, cost=None, scratch=()):
    many = isinstance(out_shape, (tuple, list))
    return pl.pallas_call(
        kernel,
        out_shape=out_shape,
        in_specs=in_specs,
        out_specs=[VMEM] * len(out_shape) if many else VMEM,
        compiler_params=pltpu.CompilerParams(vmem_limit_bytes=GRANT),
        cost_estimate=cost,
        scratch_shapes=scratch,
    )


def every_part(parts):
    return exchanged(parts.reshape(parts.shape[0], 1, LANES), ALL).reshape(parts.shape)


def on_device(embeddings, best_start, bounds_start, proposals):
    row_count, devices = embeddings.shape[0], lax.axis_size(AXIS)
    steps, props = proposals.shape
    point_total = row_count * devices

    mine, others = own_rows(pltpu.with_memory_space_constraint(proposals, pltpu.HBM), embeddings)
    half = shape_of(mine.shape, mine.dtype)
    tiles = call(pair_kernel, half, [VMEM] * 2)(mine, from_other_core(others))
    tiles = exchanged(tiles.reshape(X * Y, -1, mine.shape[1]), PLANES)
    tiles = exchanged(summed(tiles, Z), LINES)
    mine = exchanged(summed(tiles, X * Y), PLANES).reshape(mine.shape)
    others = from_other_core(mine)

    best = best_start.reshape(1, row_count)
    table = jnp.zeros((steps, LANES), jnp.float32)
    line = shape_of((devices, LANES))
    similarity, parts = call(
        functools.partial(first_kernel, props),
        [shape_of((steps * props, row_count)), line],
        [VMEM] * 4,
        scratch=[pltpu.VMEM((steps * props, mine.shape[1]), mine.dtype)],
    )(mine, others, embeddings, best)
    for step in range(steps):
        parts = every_part(parts)
        last = step == steps - 1
        best, table, parts = call(
            functools.partial(last_kernel if last else middle_kernel, step, props, point_total),
            [shape_of((1 if last else SUB, row_count)), shape_of(table.shape), line],
            [VMEM] * 4,
        )(parts, similarity, best, table)
    bounds = call(bounds_kernel, shape_of((row_count // LANES, LANES)), [SMEM, VMEM, VMEM])(
        proposals, table, bounds_start.reshape(-1, LANES)
    )
    gain_table, coverage = call(
        functools.partial(cover_kernel, props, point_total),
        [shape_of((steps, props)), shape_of((1, steps))],
        [VMEM] * 2,
    )(every_part(parts), table)
    return gain_table, coverage.reshape(-1), best.reshape(-1), bounds.reshape(-1)


def solution(mesh):
    line = Mesh(mesh.devices.reshape(-1), (AXIS,))
    in_specs = (P(AXIS, None), P(AXIS), P(AXIS), P())
    out_specs = (P(), P(), P(AXIS), P(AXIS))
    return jax.shard_map(
        on_device, mesh=line, in_specs=in_specs, out_specs=out_specs, check_vma=False
    )
```
